32 devices in a mesh: groups: 2 (over x), seq: 16 (over z, y, core).
Axes of the slice: x: 2, y: 2, z: 4, core: 2. Of those that a mesh axis runs over, the one named last changes fastest.
Arguments:
- prefill_keys: bfloat16 [128, 4096, 128], P(('groups', 'seq')), parts along dimension 0, may hold values from -4 to 4
- prefill_values: bfloat16 [128, 4096, 128], P(('groups', 'seq')), parts along dimension 0, may hold values from -6 to 6
- window_queries: bfloat16 [128, 8, 256, 128], P(('groups', 'seq')), parts along dimension 0, may hold values from -48 to 48
- step_queries: bfloat16 [128, 2, 8, 128], P('groups'), parts along dimension 0, may hold values from -48 to 48
- new_keys: bfloat16 [128, 2, 128], P('groups'), parts along dimension 0, may hold values from -24 to 24
- new_values: bfloat16 [128, 2, 128], P('groups'), parts along dimension 0, may hold values from -6 to 6
- lengths: int32 [16], P('groups'), parts along dimension 0, may hold values from 2048 to 4096
- keep_mask: int32 [16, 32], P('groups'), parts along dimension 0, may hold values from 0 to 1, as said below
Outputs:
- cache_keys: bfloat16 [128, 4096, 128], P('groups', 'seq'), parts along dimension 0
- cache_values: bfloat16 [128, 4096, 128], P('groups', 'seq'), parts along dimension 0
- attended: bfloat16 [128, 2, 8, 128], P('groups'), parts along dimension 0
- block_scores: float32 [128, 32], P('groups', 'seq'), parts along dimension 0
The draws below stay inside these ranges and needn't reach their ends.
There are 2 independent parts, one for each index of `groups`. The reference program is written for one: setup_inputs(seed, part) draws one part's arguments, and reference() takes and returns one part's arrays. A program takes and returns all parts, laid end to end along the dimension named above; each array names one. Nothing has to cross between parts.
Inputs may be any that keep to these rules, and one draw needn't show every extreme that they name: `keep_mask`: 1 keeps a block, 0 drops it; block 0 of every sequence is kept.
All inputs are finite; a program needn't handle non-finite values.
Results may differ from the reference program's by a relative error of at most 0.0055.
Values may be sent and summed in bfloat16 or wider, within the bound.
A program may use at most 128 MiB of HBM per device.

```python
import math
import jax
import jax.numpy as jnp
from jax import lax

KVH = 8
GROUP = 8
HD = 128
SEQS = 8
BLOCK = 128
WIN = 256
STEPS = 2
PAIRS = 64
LEN = 4096
NBLK = 32


def first_keys(key):
    return jnp.clip(jax.random.normal(jax.random.fold_in(key, 12), (PAIRS, HD), jnp.float32), -4.0, 4.0)


def draw_prefill_keys(key, part):
    entries = jnp.clip(jax.random.normal(jax.random.fold_in(key, 11), (PAIRS, LEN, HD), jnp.float32), -4.0, 4.0)
    return entries.at[:, 0, :].set(first_keys(key)).astype(jnp.bfloat16)


def draw_window_queries(key, part):
    sample = 3.0 * jnp.clip(jax.random.normal(jax.random.fold_in(key, 21), (PAIRS, GROUP, WIN, HD), jnp.float32), -4.0, 4.0)
    return sample.astype(jnp.bfloat16)


def plain_steps(key):
    return 3.0 * jnp.clip(jax.random.normal(jax.random.fold_in(key, 31), (PAIRS, STEPS, GROUP, HD), jnp.float32), -4.0, 4.0)


def step_sample(key):
    sample = plain_steps(key)
    return sample


def draw_step_queries(key, part):
    return step_sample(key).astype(jnp.bfloat16)


def draw_new_keys(key, part):
    centre = jnp.mean(plain_steps(key)[:, :, 1:, :].astype(jnp.bfloat16).astype(jnp.float32), axis=2)
    extra = jnp.clip(jax.random.normal(jax.random.fold_in(key, 41), (PAIRS, STEPS, HD), jnp.float32), -4.0, 4.0)
    return (centre + extra).astype(jnp.bfloat16)


def draw_keep_mask(key, part):
    picked = jax.random.randint(jax.random.fold_in(key, 51), (SEQS, NBLK), 0, 4)
    return jnp.where(picked < 3, 1, 0).astype(jnp.int32).at[:, 0].set(1)


def plant(result, stream_key, low, largest):
    longest = result.shape.index(max(result.shape))
    spots = []
    for shift in (0, 1):
        where = [jax.random.randint(jax.random.fold_in(stream_key, axis), (), 0, length) for axis, length in enumerate(result.shape)]
        where[longest] = (where[longest] + shift) % result.shape[longest]
        spots.append(tuple(where))
    return result.at[spots[0]].set(low).at[spots[1]].set(largest)


def level_of(own_key, extent, cuts, smallest, high):
    loudness = 1.0
    for dim, blocks in cuts:
        draws = jax.random.uniform(jax.random.fold_in(jax.random.fold_in(own_key, 6), dim), (blocks,), jnp.float32, smallest / len(cuts), high / len(cuts))
        loudness = loudness * jnp.repeat(jnp.exp(draws), extent[dim] // blocks).reshape((-1,) + (1,) * (len(extent) - 1 - dim))
    return loudness


def noise(key, extent, deviation, reach, shards=(), held_as=jnp.bfloat16):
    factor_of = level_of(key, extent, shards, -0.22, 0.18) if shards else 1.0
    drawn = jax.random.normal(key, extent, jnp.float32) * deviation * factor_of
    return jnp.minimum(jnp.maximum(drawn, -reach), reach).astype(held_as)


def setup_inputs(seed: int = 0, part: int = 0) -> dict:
    splits = jax.random.split(jax.random.key(seed), 9)
    part_splits = jax.random.split(jax.random.fold_in(splits[8], part), 9)
    prefill_keys = draw_prefill_keys(jax.random.fold_in(jax.random.fold_in(splits[8], part), 71), part)
    prefill_values = noise(part_splits[1], (PAIRS, LEN, HD), 1.0, 6.0, ((0, 16),))
    window_queries = draw_window_queries(jax.random.fold_in(jax.random.fold_in(splits[8], part), 71), part)
    step_queries = draw_step_queries(jax.random.fold_in(jax.random.fold_in(splits[8], part), 71), part)
    new_keys = draw_new_keys(jax.random.fold_in(jax.random.fold_in(splits[8], part), 71), part)
    new_values = noise(part_splits[5], (PAIRS, STEPS, HD), 1.0, 6.0)
    lengths = plant(jax.random.randint(part_splits[6], (SEQS,), LEN // 2, LEN + 1), jax.random.fold_in(part_splits[6], 1), LEN // 2, LEN).astype(jnp.int32)
    keep_mask = draw_keep_mask(jax.random.fold_in(jax.random.fold_in(splits[8], part), 71), part)
    return dict(prefill_keys=prefill_keys, prefill_values=prefill_values, window_queries=window_queries, step_queries=step_queries, new_keys=new_keys, new_values=new_values, lengths=lengths, keep_mask=keep_mask)


def window_prior(prefill_keys, window_queries, lengths, keep_mask):
    scaling = 1.0 / math.sqrt(HD)
    kept_tokens = jnp.repeat(keep_mask, BLOCK, axis=1) > 0
    position = jnp.arange(LEN, dtype=jnp.int32)
    offsets = jnp.tile(jnp.arange(WIN, dtype=jnp.int32), GROUP)

    def one_pair(pair_id):
        seq_id = pair_id // KVH
        query_rows = window_queries[pair_id].reshape(GROUP * WIN, HD)
        scores = jnp.dot(query_rows, prefill_keys[pair_id].T, preferred_element_type=jnp.float32) * scaling
        query_pos = lengths[seq_id] - WIN + offsets
        visible = kept_tokens[seq_id][None, :] & (position[None, :] <= query_pos[:, None])
        scores = jnp.where(visible, scores, -jnp.inf)
        highest = lax.optimization_barrier(jnp.max(scores, axis=1, keepdims=True))
        weights = jnp.exp(scores - highest)
        probability = weights / lax.optimization_barrier(jnp.sum(weights, axis=1, keepdims=True))
        return lax.optimization_barrier(jnp.sum(probability, axis=0)).reshape(NBLK, BLOCK).sum(axis=1) / GROUP
    return lax.map(one_pair, jnp.arange(PAIRS, dtype=jnp.int32))

def reference(prefill_keys, prefill_values, window_queries, step_queries, new_keys, new_values, lengths, keep_mask):
    prior_mass = window_prior(prefill_keys, window_queries, lengths, keep_mask).astype(jnp.bfloat16)
    scaling = 1.0 / math.sqrt(HD)
    position = jnp.arange(LEN, dtype=jnp.int32)
    kept_tokens = jnp.repeat(keep_mask, BLOCK, axis=1) > 0
    seq_visible = kept_tokens & (position[None, :] < lengths[:, None])
    pair_seq = jnp.arange(PAIRS, dtype=jnp.int32) // KVH
    visible = seq_visible[pair_seq]
    query_rows = step_queries.astype(jnp.float32).reshape(PAIRS, STEPS * GROUP, HD)
    scores = jnp.einsum('pqd,ptd->pqt', query_rows, prefill_keys.astype(jnp.float32), precision=lax.Precision.HIGHEST) * scaling
    scores = jnp.where(visible[:, None, :], scores, -jnp.inf)
    own_scores = jnp.einsum('pqd,pjd->pqj', query_rows, new_keys.astype(jnp.float32), precision=lax.Precision.HIGHEST) * scaling
    row_step = jnp.arange(STEPS * GROUP, dtype=jnp.int32) // GROUP
    own_visible = jnp.arange(STEPS, dtype=jnp.int32)[None, :] <= row_step[:, None]
    own_scores = jnp.where(own_visible[None], own_scores, -jnp.inf)
    highest = jnp.maximum(lax.optimization_barrier(jnp.max(scores, axis=2)), lax.optimization_barrier(jnp.max(own_scores, axis=2)))
    weights = jnp.exp(scores - highest[:, :, None])
    own_weights = jnp.exp(own_scores - highest[:, :, None])
    total_mass = lax.optimization_barrier(jnp.sum(weights, axis=2)) + lax.optimization_barrier(jnp.sum(own_weights, axis=2))
    rounded = lax.optimization_barrier(weights.astype(jnp.bfloat16)).astype(jnp.float32)
    own_rounded = lax.optimization_barrier(own_weights.astype(jnp.bfloat16)).astype(jnp.float32)
    summed = jnp.einsum('pqt,ptd->pqd', rounded, prefill_values.astype(jnp.float32), precision=lax.Precision.HIGHEST)
    summed = summed + jnp.einsum('pqj,pjd->pqd', own_rounded, new_values.astype(jnp.float32), precision=lax.Precision.HIGHEST)
    attended = (summed / total_mass[:, :, None]).astype(jnp.bfloat16).reshape(PAIRS, STEPS, GROUP, HD)
    new_mass = lax.optimization_barrier(jnp.sum(weights / total_mass[:, :, None], axis=1)).reshape(PAIRS, NBLK, BLOCK).sum(axis=2) / GROUP
    block_scores = prior_mass.astype(jnp.float32) + new_mass
    return (prefill_keys, prefill_values, attended, block_scores)
```

```python
import functools
import math

import jax
import jax.numpy as jnp
from jax import lax
from jax.experimental import pallas as pl
from jax.experimental.pallas import tpu as pltpu
from jax.sharding import PartitionSpec as P

KVH = 8
BLOCK = 128
LOW = -1e30
LIMIT = 32 * 1024 * 1024
MESH = pl.DeviceIdType.MESH


def kernel(
    n,
    chunk,
    inner,
    keys_hbm,
    values_hbm,
    window_hbm,
    queries_hbm,
    new_keys_hbm,
    new_values_hbm,
    lengths_hbm,
    keep_hbm,
    cache_keys,
    cache_values,
    attended_out,
    scores_all,
    keys,
    values,
    window,
    queries,
    new_keys,
    new_values,
    lengths_ref,
    keep_ref,
    scaled_queries,
    block_max,
    block_sum,
    mass_acc,
    attended_own,
    scores_own,
    local_sems,
    key_send,
    key_recv,
    value_send,
    value_recv,
    along_send,
    along_recv,
    across_send,
    across_recv,
    score_send,
    score_recv,
):
    group_me = lax.axis_index("groups")
    me = lax.axis_index("seq")
    pairs, tokens, width = keys_hbm.shape
    part = tokens // n
    group = window_hbm.shape[1]
    win = window_hbm.shape[2]
    steps = queries_hbm.shape[1]
    blocks = tokens // BLOCK
    first_pair = me * pairs
    scaling = 1.0 / math.sqrt(width)

    barrier = pltpu.get_barrier_semaphore()
    for k in range(1, n):
        pl.semaphore_signal(
            barrier, inc=1, device_id=(group_me, lax.rem(me + k, n)), device_id_type=MESH
        )

    loads = [
        pltpu.make_async_copy(keys_hbm, keys, local_sems.at[0]),
        pltpu.make_async_copy(values_hbm, values, local_sems.at[1]),
        pltpu.make_async_copy(window_hbm, window, local_sems.at[2]),
        pltpu.make_async_copy(queries_hbm.at[pl.ds(first_pair, pairs)], queries, local_sems.at[3]),
        pltpu.make_async_copy(new_keys_hbm.at[pl.ds(first_pair, pairs)], new_keys, local_sems.at[4]),
        pltpu.make_async_copy(
            new_values_hbm.at[pl.ds(first_pair, pairs)], new_values, local_sems.at[5]
        ),
        pltpu.make_async_copy(
            keys_hbm.at[:, pl.ds(me * part, part), :],
            cache_keys.at[pl.ds(first_pair, pairs)],
            local_sems.at[6],
        ),
        pltpu.make_async_copy(
            values_hbm.at[:, pl.ds(me * part, part), :],
            cache_values.at[pl.ds(first_pair, pairs)],
            local_sems.at[7],
        ),
        pltpu.make_async_copy(lengths_hbm, lengths_ref, local_sems.at[8]),
        pltpu.make_async_copy(keep_hbm, keep_ref, local_sems.at[9]),
    ]
    for load in loads:
        load.start()
    pl.semaphore_wait(barrier, n - 1)

    def remote(src, dst, send, recv, k):
        return pltpu.make_async_remote_copy(
            src_ref=src,
            dst_ref=dst,
            send_sem=send.at[k],
            recv_sem=recv.at[k],
            device_id=(group_me, lax.rem(me + k, n)),
            device_id_type=MESH,
        )

    sends = []
    for src, dst, send, recv in (
        (keys_hbm, cache_keys, key_send, key_recv),
        (values_hbm, cache_values, value_send, value_recv),
    ):
        for k in range(1, n):
            peer = lax.rem(me + k, n)
            sends.append(
                remote(
                    src.at[:, pl.ds(peer * part, part), :],
                    dst.at[pl.ds(first_pair, pairs)],
                    send,
                    recv,
                    k,
                )
            )
    for copy in sends[: n - 1]:
        copy.start()
    for load in loads:
        load.wait()

    lanes = lax.broadcasted_iota(jnp.int32, (1, BLOCK), 1)
    scores_own[...] = jnp.zeros_like(scores_own)

    def decode(p, carry):
        seq_id = (first_pair + p) // KVH
        length = lengths_ref[seq_id]
        rows = queries[p].reshape(steps * group, width)
        scores = (
            lax.dot_general(
                rows, keys[p], (((1,), (1,)), ((), ())), preferred_element_type=jnp.float32
            )
            * scaling
        )
        limits = []
        for b in range(blocks):
            limit = jnp.where(keep_ref[seq_id, b] > 0, length - b * BLOCK, 0)
            limits.append(lanes < limit)
        visible = jnp.concatenate([jnp.where(v, 0.0, -jnp.inf) for v in limits], axis=1)
        scores = scores + visible
        rows32 = rows.astype(jnp.float32)
        row_step = lax.broadcasted_iota(jnp.int32, (steps * group, 1), 0) // group
        own = []
        highest = jnp.max(scores, axis=1, keepdims=True)
        for j in range(steps):
            key_row = new_keys[p, j : j + 1].astype(jnp.float32)
            own_j = jnp.sum(rows32 * key_row, axis=1, keepdims=True) * scaling
            own_j = jnp.where(j <= row_step, own_j, -jnp.inf)
            own.append(own_j)
            highest = jnp.maximum(highest, own_j)
        weights = jnp.exp(scores - highest)
        total = jnp.sum(weights, axis=1, keepdims=True)
        summed = jnp.dot(
            weights.astype(jnp.bfloat16), values[p], preferred_element_type=jnp.float32
        )
        for j in range(steps):
            own_weight = jnp.exp(own[j] - highest)
            total = total + own_weight
            value_row = new_values[p, j : j + 1].astype(jnp.float32)
            summed = summed + own_weight.astype(jnp.bfloat16).astype(jnp.float32) * value_row
        attended_own[p] = (summed / total).astype(jnp.bfloat16).reshape(steps, group, width)
        mass = jnp.sum(weights / total, axis=0, keepdims=True) / group
        line = jnp.zeros((1, BLOCK), jnp.float32)
        for b in range(blocks):
            piece = jnp.sum(mass[:, b * BLOCK : (b + 1) * BLOCK], axis=1, keepdims=True)
            line = line + jnp.where(lanes == b, piece, 0.0)
        scores_own[pl.ds(p, 1), :] = line
        return carry

    lax.fori_loop(0, pairs, decode, 0)

    row, column = me // inner, lax.rem(me, inner)
    rows = n // inner
    along = []
    for i in range(1, rows):
        along.append(
            pltpu.make_async_remote_copy(
                src_ref=attended_own,
                dst_ref=attended_out.at[pl.ds(first_pair, pairs)],
                send_sem=along_send.at[i],
                recv_sem=along_recv.at[i],
                device_id=(group_me, lax.rem(row + i, rows) * inner + column),
                device_id_type=MESH,
            )
        )
    for copy in along:
        copy.start()
    late = len(sends)
    for copy in sends[n - 1 : late]:
        copy.start()

    factor = scaling * math.log2(math.e)
    per_chunk = chunk // BLOCK
    gap = lax.broadcasted_iota(jnp.int32, (BLOCK, win), 1) - lax.broadcasted_iota(
        jnp.int32, (BLOCK, win), 0
    )
    row_block = lax.broadcasted_iota(jnp.int32, (blocks * 8, BLOCK), 0) // 8
    in_block = row_block == lax.broadcasted_iota(jnp.int32, (blocks * 8, BLOCK), 1)

    def one_pair(p, carry):
        seq_id = (first_pair + p) // KVH
        start = lengths_ref[seq_id] - win
        mass_acc[...] = jnp.zeros_like(mass_acc)

        def one_head(g, carry):
            wide = window[p, g].astype(jnp.float32) * factor
            high = wide.astype(jnp.bfloat16)
            low = (wide - high.astype(jnp.float32)).astype(jnp.bfloat16)
            scaled_queries[...] = jnp.concatenate([high.T, low.T], axis=0)

            def one_chunk(c, carry):
                base = pl.multiple_of(c * chunk, chunk)
                tile = keys[p, pl.ds(base, chunk), :]
                doubled = jnp.concatenate([tile, tile], axis=1)
                scores = jnp.dot(doubled, scaled_queries[...], preferred_element_type=jnp.float32)
                for i in range(per_chunk):
                    b = c * per_chunk + i
                    part_scores = jnp.where(
                        gap >= b * BLOCK - start, scores[i * BLOCK : (i + 1) * BLOCK], LOW
                    )
                    stacked = part_scores.reshape(BLOCK // 8, 8, win)
                    top = jnp.max(stacked, axis=0)
                    total = jnp.sum(jnp.exp2(stacked - top[None]), axis=0)
                    kept = keep_ref[seq_id, b] > 0
                    spot = pl.ds(pl.multiple_of(b * 8, 8), 8)
                    block_max[spot, :] = jnp.where(kept, top, LOW)
                    block_sum[spot, :] = jnp.where(kept, total, 0.0)
                return carry

            lax.fori_loop(0, tokens // chunk, one_chunk, 0)
            highest = jnp.max(block_max[...], axis=0, keepdims=True)
            shares = block_sum[...] * jnp.exp2(block_max[...] - highest)
            mass_acc[...] += shares / jnp.sum(shares, axis=0, keepdims=True)
            return carry

        lax.fori_loop(0, group, one_head, 0)
        row_mass = jnp.sum(mass_acc[...], axis=1, keepdims=True)
        prior = jnp.sum(jnp.where(in_block, row_mass, 0.0), axis=0, keepdims=True) / group
        line = prior.astype(jnp.bfloat16).astype(jnp.float32)
        scores_own[pl.ds(p, 1), :] = scores_own[pl.ds(p, 1), :] + line
        return carry

    lax.fori_loop(0, pairs, one_pair, 0)

    small = [
        remote(scores_own, scores_all.at[me], score_send, score_recv, k) for k in range(1, n)
    ]
    for copy in small:
        copy.start()
    for copy in along:
        copy.wait()
    across = []
    for i in range(rows):
        source = lax.rem(row + rows - i, rows) * inner + column
        spot = pl.ds(source * pairs, pairs)
        for j in range(1, inner):
            across.append(
                pltpu.make_async_remote_copy(
                    src_ref=attended_own if i == 0 else attended_out.at[spot],
                    dst_ref=attended_out.at[spot],
                    send_sem=across_send.at[i * inner + j],
                    recv_sem=across_recv.at[i * inner + j],
                    device_id=(group_me, row * inner + lax.rem(column + j, inner)),
                    device_id_type=MESH,
                )
            )
    for copy in across:
        copy.start()
    for copy in sends[late:]:
        copy.start()
    kept_here = [
        pltpu.make_async_copy(
            attended_own, attended_out.at[pl.ds(first_pair, pairs)], local_sems.at[0]
        ),
        pltpu.make_async_copy(scores_own, scores_all.at[me], local_sems.at[1]),
    ]
    for copy in kept_here:
        copy.start()
    for copy in kept_here:
        copy.wait()
    for copy in small:
        copy.wait()
    for copy in across:
        copy.wait()
    for copy in sends:
        copy.wait()


def settle(n, pieces, keys, values, attended, scores, *rest):
    cache_keys, cache_values, attended_out, scores_out, sems = rest
    me = lax.axis_index("seq")
    here = scores_out.shape[0]
    step = keys.shape[0] // pieces
    stores = []
    for source, target in ((keys, cache_keys), (values, cache_values)):
        for i in range(pieces):
            spot = pl.ds(i * step, step)
            stores.append(
                pltpu.make_async_copy(source.at[spot], target.at[spot], sems.at[len(stores)])
            )
    stores.append(pltpu.make_async_copy(attended, attended_out, sems.at[len(stores)]))
    for store in stores:
        store.start()
    flat = scores[...].reshape(scores.shape[0] * scores.shape[1], BLOCK)
    turned = pltpu.roll(flat, lax.rem(BLOCK - me * here, BLOCK), 1)
    scores_out[...] = turned.T[:here]
    for store in stores:
        store.wait()


def local(n, *args):
    keys, values, window, queries, new_keys, new_values, lengths, keep = args
    pairs, tokens, width = keys.shape
    part = tokens // n
    blocks = tokens // BLOCK
    win = window.shape[2]
    every = n * pairs
    inner = 4 if n % 4 == 0 else 1
    vmem = pl.BlockSpec(memory_space=pltpu.VMEM)
    hbm = pl.BlockSpec(memory_space=pltpu.HBM)
    free = pl.BlockSpec(memory_space=pl.ANY)
    bf16, f32 = jnp.bfloat16, jnp.float32
    moved = pl.pallas_call(
        functools.partial(kernel, n, min(512, tokens), inner),
        out_shape=(
            pltpu.VMEM((every, part, width), bf16),
            pltpu.VMEM((every, part, width), bf16),
            pltpu.VMEM((every,) + queries.shape[1:], bf16),
            pltpu.VMEM((n, pairs, BLOCK), f32),
        ),
        in_specs=[hbm] * 8,
        out_specs=(vmem,) * 4,
        scratch_shapes=[
            pltpu.VMEM(keys.shape, bf16),
            pltpu.VMEM(values.shape, bf16),
            pltpu.VMEM(window.shape, bf16),
            pltpu.VMEM((pairs,) + queries.shape[1:], bf16),
            pltpu.VMEM((pairs,) + new_keys.shape[1:], bf16),
            pltpu.VMEM((pairs,) + new_values.shape[1:], bf16),
            pltpu.SMEM(lengths.shape, jnp.int32),
            pltpu.SMEM(keep.shape, jnp.int32),
            pltpu.VMEM((2 * width, win), bf16),
            pltpu.VMEM((blocks * 8, win), f32),
            pltpu.VMEM((blocks * 8, win), f32),
            pltpu.VMEM((blocks * 8, win), f32),
            pltpu.VMEM((pairs,) + queries.shape[1:], bf16),
            pltpu.VMEM((pairs, BLOCK), f32),
            pltpu.SemaphoreType.DMA((10,)),
        ]
        + [pltpu.SemaphoreType.DMA((n,))] * 10,
        compiler_params=pltpu.CompilerParams(
            collective_id=0, has_side_effects=True, vmem_limit_bytes=LIMIT
        ),
    )(*(pltpu.with_memory_space_constraint(a, pltpu.HBM) for a in args))
    pieces = math.gcd(every, 8)
    cache_keys, cache_values, attended, scores = pl.pallas_call(
        functools.partial(settle, n, pieces),
        out_shape=(
            jax.ShapeDtypeStruct((every, part, width), bf16),
            jax.ShapeDtypeStruct((every, part, width), bf16),
            jax.ShapeDtypeStruct((every,) + queries.shape[1:], bf16),
            jax.ShapeDtypeStruct((part // BLOCK, every), f32),
        ),
        in_specs=[vmem] * 4,
        out_specs=(free, free, free, vmem),
        scratch_shapes=[pltpu.SemaphoreType.DMA((2 * pieces + 1,))],
        compiler_params=pltpu.CompilerParams(vmem_limit_bytes=LIMIT),
    )(*moved)
    return cache_keys, cache_values, attended, scores.T


def solution(mesh):
    placed = (
        P(("groups", "seq"), None, None),
        P(("groups", "seq"), None, None),
        P(("groups", "seq"), None, None, None),
        P("groups", None, None, None),
        P("groups", None, None),
        P("groups", None, None),
        P("groups"),
        P("groups", None),
    )
    return jax.shard_map(
        functools.partial(local, mesh.shape["seq"]),
        mesh=mesh,
        in_specs=placed,
        out_specs=(
            P("groups", "seq", None),
            P("groups", "seq", None),
            P("groups", None, None, None),
            P("groups", "seq"),
        ),
        check_vma=False,
    )
```

```python
import functools
import math

import jax
import jax.numpy as jnp
from jax import lax
from jax.experimental import pallas as pl
from jax.experimental.pallas import tpu as pltpu
from jax.sharding import PartitionSpec as P

KVH = 8
BLOCK = 128
LOW = -1e30
LIMIT = 32 * 1024 * 1024
MESH = pl.DeviceIdType.MESH


def kernel(
    n,
    chunk,
    inner,
    keys_hbm,
    values_hbm,
    window_hbm,
    queries_hbm,
    new_keys_hbm,
    new_values_hbm,
    lengths_hbm,
    keep_hbm,
    cache_keys,
    cache_values,
    attended_out,
    scores_all,
    keys,
    values,
    window,
    queries,
    new_keys,
    new_values,
    lengths_ref,
    keep_ref,
    scaled_queries,
    block_max,
    block_sum,
    mass_acc,
    attended_own,
    scores_own,
    local_sems,
    present,
    up_send,
    up_recv,
    down_send,
    down_recv,
    near_send,
    near_recv,
    along_send,
    along_recv,
    relay_send,
    relay_recv,
    across_send,
    across_recv,
):
    group_me = lax.axis_index("groups")
    me = lax.axis_index("seq")
    pairs, tokens, width = keys_hbm.shape
    part = tokens // n
    group = window_hbm.shape[1]
    win = window_hbm.shape[2]
    steps = queries_hbm.shape[1]
    blocks = tokens // BLOCK
    first_pair = me * pairs
    scaling = 1.0 / math.sqrt(width)
    rows = n // inner
    row, column = me // inner, lax.rem(me, inner)

    barrier = pltpu.get_barrier_semaphore()
    for k in range(1, n):

        @pl.when(me + k < n)
        def _():
            pl.semaphore_signal(
                barrier, inc=1, device_id=(group_me, me + k), device_id_type=MESH
            )

    loads = [
        pltpu.make_async_copy(keys_hbm, keys, local_sems.at[0]),
        pltpu.make_async_copy(values_hbm, values, local_sems.at[1]),
        pltpu.make_async_copy(window_hbm, window, local_sems.at[2]),
        pltpu.make_async_copy(queries_hbm.at[pl.ds(first_pair, pairs)], queries, local_sems.at[3]),
        pltpu.make_async_copy(new_keys_hbm.at[pl.ds(first_pair, pairs)], new_keys, local_sems.at[4]),
        pltpu.make_async_copy(
            new_values_hbm.at[pl.ds(first_pair, pairs)], new_values, local_sems.at[5]
        ),
        pltpu.make_async_copy(
            keys_hbm.at[:, pl.ds(me * part, part), :],
            cache_keys.at[pl.ds(first_pair, pairs)],
            local_sems.at[6],
        ),
        pltpu.make_async_copy(
            values_hbm.at[:, pl.ds(me * part, part), :],
            cache_values.at[pl.ds(first_pair, pairs)],
            local_sems.at[7],
        ),
        pltpu.make_async_copy(lengths_hbm, lengths_ref, local_sems.at[8]),
        pltpu.make_async_copy(keep_hbm, keep_ref, local_sems.at[9]),
    ]

    @pl.when(me > 0)
    def _():
        pl.semaphore_wait(barrier, me)

    for k in range(1, n):

        @pl.when(me >= k)
        def _():
            pl.semaphore_signal(
                present.at[me], inc=1, device_id=(group_me, me - k), device_id_type=MESH
            )

    if inner == 4:
        flip = 2 * lax.rem(column, 2)
        turns = [flip, 2 - flip, 1 + flip, 3 - flip]
    else:
        turns = list(range(inner))

    def move(which, target, spot, send, recv):
        src, dst = ((keys_hbm, cache_keys), (values_hbm, cache_values))[which]
        return pltpu.make_async_remote_copy(
            src_ref=src.at[:, pl.ds(target * part, part), :],
            dst_ref=dst.at[pl.ds(first_pair, pairs)],
            send_sem=send.at[which, spot],
            recv_sem=recv.at[which, spot],
            device_id=(group_me, target),
            device_id_type=MESH,
        )

    def down(which, distance, c):
        target = lax.rem(row - distance + rows, rows) * inner + (column ^ c)
        return move(which, target, distance * inner + c, down_send, down_recv)

    def up(which, distance, c):
        target = lax.rem(row + distance, rows) * inner + (column ^ c)
        return move(which, target, distance * inner + c, up_send, up_recv)

    def near(which, c):
        return move(which, row * inner + (column ^ c), c, near_send, near_recv)

    def start_down(distance, kinds):
        for which in kinds:
            for c in turns:
                down(which, distance, c).start()

    def start_up(distance, kinds):
        for which in kinds:
            for c in turns:
                up(which, distance, c).start()

    def await_up(distance, c):
        pl.semaphore_wait(present.at[(row + distance) * inner + (column ^ c)], 1)

    @pl.when(row > 0)
    def _():
        start_down(row, (0, 1))

    for u in range(1, rows - 1):

        @pl.when(u < row - 1)
        def _():
            start_down(u, (0, 1))

        @pl.when(u == row - 1)
        def _():
            start_down(u, (0,))

    early = [2 * (column // 2) ^ c for c in range(inner)] if inner == 4 else list(range(inner))
    for u in range(1, rows):

        @pl.when(row + u < rows)
        def _():
            for c in early:
                await_up(u, c)
                if u > 1:
                    up(0, u, c).start()
                else:

                    @pl.when(row > 0)
                    def _():
                        up(0, u, c).start()

        if u > 1:

            @pl.when((row == 0) & (row + u < rows))
            def _():
                start_up(u, (1,))

    for load in loads:
        load.start()
    for c in range(1, inner):

        @pl.when((column ^ c) > column)
        def _():
            pl.semaphore_wait(present.at[row * inner + (column ^ c)], 1)

        for which in (0, 1):
            near(which, c).start()

    def start_rest():
        @pl.when(row > 1)
        def _():
            start_down(row - 1, (1,))

        for u in range(rows - 1, 0, -1):

            @pl.when((row > 0) & (row + u < rows))
            def _():
                start_up(u, (1,))

        if rows > 1:

            @pl.when(row == 0)
            def _():
                start_up(1, (0, 1))

    for load in loads:
        load.wait()

    lanes = lax.broadcasted_iota(jnp.int32, (1, BLOCK), 1)
    scores_own[...] = jnp.zeros_like(scores_own)

    def decode(p, carry):
        seq_id = (first_pair + p) // KVH
        length = lengths_ref[seq_id]
        rows = queries[p].reshape(steps * group, width)
        scores = (
            lax.dot_general(
                rows, keys[p], (((1,), (1,)), ((), ())), preferred_element_type=jnp.float32
            )
            * scaling
        )
        limits = []
        for b in range(blocks):
            limit = jnp.where(keep_ref[seq_id, b] > 0, length - b * BLOCK, 0)
            limits.append(lanes < limit)
        visible = jnp.concatenate([jnp.where(v, 0.0, -jnp.inf) for v in limits], axis=1)
        scores = scores + visible
        rows32 = rows.astype(jnp.float32)
        row_step = lax.broadcasted_iota(jnp.int32, (steps * group, 1), 0) // group
        own = []
        highest = jnp.max(scores, axis=1, keepdims=True)
        for j in range(steps):
            key_row = new_keys[p, j : j + 1].astype(jnp.float32)
            own_j = jnp.sum(rows32 * key_row, axis=1, keepdims=True) * scaling
            own_j = jnp.where(j <= row_step, own_j, -jnp.inf)
            own.append(own_j)
            highest = jnp.maximum(highest, own_j)
        weights = jnp.exp(scores - highest)
        total = jnp.sum(weights, axis=1, keepdims=True)
        summed = jnp.dot(
            weights.astype(jnp.bfloat16), values[p], preferred_element_type=jnp.float32
        )
        for j in range(steps):
            own_weight = jnp.exp(own[j] - highest)
            total = total + own_weight
            value_row = new_values[p, j : j + 1].astype(jnp.float32)
            summed = summed + own_weight.astype(jnp.bfloat16).astype(jnp.float32) * value_row
        attended_own[p] = (summed / total).astype(jnp.bfloat16).reshape(steps, group, width)
        mass = jnp.sum(weights / total, axis=0, keepdims=True) / group
        line = jnp.zeros((1, BLOCK), jnp.float32)
        for b in range(blocks):
            piece = jnp.sum(mass[:, b * BLOCK : (b + 1) * BLOCK], axis=1, keepdims=True)
            line = line + jnp.where(lanes == b, piece, 0.0)
        scores_own[pl.ds(p, 1), :] = line
        return carry

    lax.fori_loop(0, pairs, decode, 0)

    factor = scaling * math.log2(math.e)
    per_chunk = chunk // BLOCK
    gap = lax.broadcasted_iota(jnp.int32, (BLOCK, win), 1) - lax.broadcasted_iota(
        jnp.int32, (BLOCK, win), 0
    )
    row_block = lax.broadcasted_iota(jnp.int32, (blocks * 8, BLOCK), 0) // 8
    in_block = row_block == lax.broadcasted_iota(jnp.int32, (blocks * 8, BLOCK), 1)

    def one_pair(p, carry):
        seq_id = (first_pair + p) // KVH
        start = lengths_ref[seq_id] - win
        mass_acc[...] = jnp.zeros_like(mass_acc)

        def one_head(g, carry):
            wide = window[p, g].astype(jnp.float32) * factor
            high = wide.astype(jnp.bfloat16)
            low = (wide - high.astype(jnp.float32)).astype(jnp.bfloat16)
            scaled_queries[...] = jnp.concatenate([high.T, low.T], axis=0)

            def one_chunk(c, carry):
                base = pl.multiple_of(c * chunk, chunk)
                tile = keys[p, pl.ds(base, chunk), :]
                doubled = jnp.concatenate([tile, tile], axis=1)
                scores = jnp.dot(doubled, scaled_queries[...], preferred_element_type=jnp.float32)
                for i in range(per_chunk):
                    b = c * per_chunk + i
                    part_scores = jnp.where(
                        gap >= b * BLOCK - start, scores[i * BLOCK : (i + 1) * BLOCK], LOW
                    )
                    stacked = part_scores.reshape(BLOCK // 8, 8, win)
                    top = jnp.max(stacked, axis=0)
                    total = jnp.sum(jnp.exp2(stacked - top[None]), axis=0)
                    kept = keep_ref[seq_id, b] > 0
                    spot = pl.ds(pl.multiple_of(b * 8, 8), 8)
                    block_max[spot, :] = jnp.where(kept, top, LOW)
                    block_sum[spot, :] = jnp.where(kept, total, 0.0)
                return carry

            lax.fori_loop(0, tokens // chunk, one_chunk, 0)
            highest = jnp.max(block_max[...], axis=0, keepdims=True)
            shares = block_sum[...] * jnp.exp2(block_max[...] - highest)
            mass_acc[...] += shares / jnp.sum(shares, axis=0, keepdims=True)
            return carry

        lax.fori_loop(0, group, one_head, 0)
        row_mass = jnp.sum(mass_acc[...], axis=1, keepdims=True)
        prior = jnp.sum(jnp.where(in_block, row_mass, 0.0), axis=0, keepdims=True) / group
        line = prior.astype(jnp.bfloat16).astype(jnp.float32)
        scores_own[pl.ds(p, 1), :] = scores_own[pl.ds(p, 1), :] + line
        return carry

    lax.fori_loop(0, pairs, one_pair, 0)

    results = ((attended_own, attended_out), (scores_own, scores_all))
    half = rows // 2
    low = row < half

    def along(i, u):
        own, landing = results[i]
        return pltpu.make_async_remote_copy(
            src_ref=own,
            dst_ref=landing.at[row, column],
            send_sem=along_send.at[i, u],
            recv_sem=along_recv.at[i, u],
            device_id=(group_me, lax.rem(row + u, rows) * inner + column),
            device_id_type=MESH,
        )

    def relay(i, upward, target):
        landing = results[i][1]
        block = landing.at[pl.ds(0, half) if upward else pl.ds(half, rows - half), column]
        return pltpu.make_async_remote_copy(
            src_ref=block,
            dst_ref=block,
            send_sem=relay_send.at[i, target],
            recv_sem=relay_recv.at[i],
            device_id=(group_me, target * inner + column),
            device_id_type=MESH,
        )

    across = [
        pltpu.make_async_remote_copy(
            src_ref=landing.at[:, column],
            dst_ref=landing.at[:, column],
            send_sem=across_send.at[i, c],
            recv_sem=across_recv.at[i, c],
            device_id=(group_me, row * inner + (column ^ c)),
            device_id_type=MESH,
        )
        for c in range(1, inner)
        for i, (own, landing) in enumerate(results)
    ]
    kept_here = [
        pltpu.make_async_copy(own, landing.at[row, column], local_sems.at[i])
        for i, (own, landing) in enumerate(results)
    ]
    for u in range(1, rows):
        target = lax.rem(row + u, rows)

        @pl.when((low == (target < half)) | (target == jnp.where(low, half, half - 1)))
        def _():
            for i in range(2):
                along(i, u).start()

    start_rest()
    for copy in kept_here:
        copy.start()
    for copy in kept_here:
        copy.wait()
    for u in range(1, rows):
        source = lax.rem(row + rows - u, rows)

        @pl.when((low == (source < half)) | (row == jnp.where(source < half, half, half - 1)))
        def _():
            for i in range(2):
                along(i, u).wait_recv()

    upper, lower = range(half + 1, rows), range(0, half - 1)
    for upward, gate, targets in ((True, half, upper), (False, half - 1, lower)):
        for target in targets:

            @pl.when(row == gate)
            def _():
                for i in range(2):
                    relay(i, upward, target).start()

            @pl.when(row == target)
            def _():
                for i in range(2):
                    relay(i, upward, target).wait_recv()

    for copy in across:
        copy.start()
    for copy in across:
        copy.wait()
    for upward, gate, targets in ((True, half, upper), (False, half - 1, lower)):
        for target in targets:

            @pl.when(row == gate)
            def _():
                for i in range(2):
                    relay(i, upward, target).wait_send()

    for u in range(1, rows):
        target = lax.rem(row + u, rows)

        @pl.when((low == (target < half)) | (target == jnp.where(low, half, half - 1)))
        def _():
            for i in range(2):
                along(i, u).wait_send()

    for c in range(1, inner):
        for which in (0, 1):
            near(which, c).wait()
    for u in range(1, rows):
        for make, sends, receives in (
            (down, row >= u, row + u < rows),
            (up, row + u < rows, row >= u),
        ):

            @pl.when(sends)
            def _():
                for which in (0, 1):
                    for c in range(inner):
                        make(which, u, c).wait_send()

            @pl.when(receives)
            def _():
                for which in (0, 1):
                    for c in range(inner):
                        make(which, u, c).wait_recv()


def settle(n, pieces, keys, values, attended, scores, *rest):
    cache_keys, cache_values, attended_out, scores_out, sems = rest
    me = lax.axis_index("seq")
    here = scores_out.shape[0]
    step = keys.shape[0] // pieces
    stores = []
    for source, target in ((keys, cache_keys), (values, cache_values)):
        for i in range(pieces):
            spot = pl.ds(i * step, step)
            stores.append(
                pltpu.make_async_copy(source.at[spot], target.at[spot], sems.at[len(stores)])
            )
    stores.append(pltpu.make_async_copy(attended, attended_out, sems.at[len(stores)]))
    for store in stores:
        store.start()
    flat = scores[...].reshape(math.prod(scores.shape[:-1]), BLOCK)
    turned = pltpu.roll(flat, lax.rem(BLOCK - me * here, BLOCK), 1)
    scores_out[...] = turned.T[:here]
    for store in stores:
        store.wait()


def local(n, *args):
    keys, values, window, queries, new_keys, new_values, lengths, keep = args
    pairs, tokens, width = keys.shape
    part = tokens // n
    blocks = tokens // BLOCK
    win = window.shape[2]
    every = n * pairs
    inner = 4 if n % 4 == 0 else 1
    vmem = pl.BlockSpec(memory_space=pltpu.VMEM)
    hbm = pl.BlockSpec(memory_space=pltpu.HBM)
    free = pl.BlockSpec(memory_space=pl.ANY)
    bf16, f32 = jnp.bfloat16, jnp.float32
    moved = pl.pallas_call(
        functools.partial(kernel, n, min(512, tokens), inner),
        out_shape=(
            pltpu.VMEM((every, part, width), bf16),
            pltpu.VMEM((every, part, width), bf16),
            pltpu.VMEM((n // inner, inner, pairs) + queries.shape[1:], bf16),
            pltpu.VMEM((n // inner, inner, pairs, BLOCK), f32),
        ),
        in_specs=[hbm] * 8,
        out_specs=(vmem,) * 4,
        scratch_shapes=[
            pltpu.VMEM(keys.shape, bf16),
            pltpu.VMEM(values.shape, bf16),
            pltpu.VMEM(window.shape, bf16),
            pltpu.VMEM((pairs,) + queries.shape[1:], bf16),
            pltpu.VMEM((pairs,) + new_keys.shape[1:], bf16),
            pltpu.VMEM((pairs,) + new_values.shape[1:], bf16),
            pltpu.SMEM(lengths.shape, jnp.int32),
            pltpu.SMEM(keep.shape, jnp.int32),
            pltpu.VMEM((2 * width, win), bf16),
            pltpu.VMEM((blocks * 8, win), f32),
            pltpu.VMEM((blocks * 8, win), f32),
            pltpu.VMEM((blocks * 8, win), f32),
            pltpu.VMEM((pairs,) + queries.shape[1:], bf16),
            pltpu.VMEM((pairs, BLOCK), f32),
            pltpu.SemaphoreType.DMA((10,)),
        ]
        + [pltpu.SemaphoreType.REGULAR((n,))]
        + [pltpu.SemaphoreType.DMA((2, n))] * 4
        + [pltpu.SemaphoreType.DMA((2, inner))] * 2
        + [pltpu.SemaphoreType.DMA((2, n))] * 3
        + [pltpu.SemaphoreType.DMA((2,))]
        + [pltpu.SemaphoreType.DMA((2, n))] * 2,
        compiler_params=pltpu.CompilerParams(
            collective_id=0, has_side_effects=True, vmem_limit_bytes=LIMIT
        ),
    )(*(pltpu.with_memory_space_constraint(a, pltpu.HBM) for a in args))
    pieces = math.gcd(every, 8)
    cache_keys, cache_values, attended, scores = pl.pallas_call(
        functools.partial(settle, n, pieces),
        out_shape=(
            jax.ShapeDtypeStruct((every, part, width), bf16),
            jax.ShapeDtypeStruct((every, part, width), bf16),
            jax.ShapeDtypeStruct(moved[2].shape, bf16),
            jax.ShapeDtypeStruct((part // BLOCK, every), f32),
        ),
        in_specs=[vmem] * 4,
        out_specs=(free, free, free, vmem),
        scratch_shapes=[pltpu.SemaphoreType.DMA((2 * pieces + 1,))],
        compiler_params=pltpu.CompilerParams(vmem_limit_bytes=LIMIT),
    )(*moved)
    return cache_keys, cache_values, attended.reshape((every,) + queries.shape[1:]), scores.T


def solution(mesh):
    placed = (
        P(("groups", "seq"), None, None),
        P(("groups", "seq"), None, None),
        P(("groups", "seq"), None, None, None),
        P("groups", None, None, None),
        P("groups", None, None),
        P("groups", None, None),
        P("groups"),
        P("groups", None),
    )
    return jax.shard_map(
        functools.partial(local, mesh.shape["seq"]),
        mesh=mesh,
        in_specs=placed,
        out_specs=(
            P("groups", "seq", None),
            P("groups", "seq", None),
            P("groups", None, None, None),
            P("groups", "seq"),
        ),
        check_vma=False,
    )
```

```python
import functools
import math

import jax
import jax.numpy as jnp
from jax import lax
from jax.experimental import pallas as pl
from jax.experimental.pallas import tpu as pltpu
from jax.sharding import PartitionSpec as P

KVH = 8
BLOCK = 128
LOW = -1e30
LIMIT = 32 * 1024 * 1024
MESH = pl.DeviceIdType.MESH


def kernel(
    n,
    chunk,
    inner,
    keys_hbm,
    values_hbm,
    window_hbm,
    queries_hbm,
    new_keys_hbm,
    new_values_hbm,
    lengths_hbm,
    keep_hbm,
    cache_keys,
    cache_values,
    attended_out,
    scores_all,
    keys,
    values,
    window,
    queries,
    new_keys,
    new_values,
    lengths_ref,
    keep_ref,
    scaled_queries,
    block_max,
    block_sum,
    mass_acc,
    attended_own,
    scores_own,
    local_sems,
    present,
    up_send,
    up_recv,
    down_send,
    down_recv,
    near_send,
    near_recv,
    along_send,
    along_recv,
    relay_send,
    relay_recv,
    across_send,
    across_recv,
):
    group_me = lax.axis_index("groups")
    me = lax.axis_index("seq")
    pairs, tokens, width = keys_hbm.shape
    part = tokens // n
    group = window_hbm.shape[1]
    win = window_hbm.shape[2]
    steps = queries_hbm.shape[1]
    blocks = tokens // BLOCK
    first_pair = me * pairs
    scaling = 1.0 / math.sqrt(width)
    rows = n // inner
    row, column = me // inner, lax.rem(me, inner)

    half = rows // 2
    gate_low, gate_high = half - 1, half
    barrier = pltpu.get_barrier_semaphore()
    for k in range(1, n):

        @pl.when(me + k < n)
        def _():
            pl.semaphore_signal(
                barrier, inc=1, device_id=(group_me, me + k), device_id_type=MESH
            )

    loads = [
        pltpu.make_async_copy(keys_hbm, keys, local_sems.at[0]),
        pltpu.make_async_copy(values_hbm, values, local_sems.at[1]),
        pltpu.make_async_copy(window_hbm, window, local_sems.at[2]),
        pltpu.make_async_copy(queries_hbm.at[pl.ds(first_pair, pairs)], queries, local_sems.at[3]),
        pltpu.make_async_copy(new_keys_hbm.at[pl.ds(first_pair, pairs)], new_keys, local_sems.at[4]),
        pltpu.make_async_copy(
            new_values_hbm.at[pl.ds(first_pair, pairs)], new_values, local_sems.at[5]
        ),
        pltpu.make_async_copy(
            keys_hbm.at[:, pl.ds(me * part, part), :],
            cache_keys.at[pl.ds(first_pair, pairs)],
            local_sems.at[6],
        ),
        pltpu.make_async_copy(
            values_hbm.at[:, pl.ds(me * part, part), :],
            cache_values.at[pl.ds(first_pair, pairs)],
            local_sems.at[7],
        ),
        pltpu.make_async_copy(lengths_hbm, lengths_ref, local_sems.at[8]),
        pltpu.make_async_copy(keep_hbm, keep_ref, local_sems.at[9]),
    ]
    if rows > 1:

        @pl.when(row == gate_high)
        def _():
            for c in range(inner):
                pl.semaphore_signal(
                    barrier, inc=1, device_id=(group_me, gate_low * inner + c), device_id_type=MESH
                )

        @pl.when(row == gate_low)
        def _():
            pl.semaphore_wait(barrier, me + inner)

    @pl.when((me > 0) & (row != gate_low))
    def _():
        pl.semaphore_wait(barrier, me)

    for k in range(1, n):

        @pl.when((me >= k) & ((row != gate_high) | ((me - k) // inner != gate_low)))
        def _():
            pl.semaphore_signal(
                present.at[me], inc=1, device_id=(group_me, me - k), device_id_type=MESH
            )

    if inner == 4:
        flip = 2 * lax.rem(column, 2)
        turns = [flip, 2 - flip, 1 + flip, 3 - flip]
    else:
        turns = list(range(inner))

    def move(which, target, spot, send, recv):
        src, dst = ((keys_hbm, cache_keys), (values_hbm, cache_values))[which]
        return pltpu.make_async_remote_copy(
            src_ref=src.at[:, pl.ds(target * part, part), :],
            dst_ref=dst.at[pl.ds(first_pair, pairs)],
            send_sem=send.at[which, spot],
            recv_sem=recv.at[which, spot],
            device_id=(group_me, target),
            device_id_type=MESH,
        )

    def down(which, distance, c):
        target = lax.rem(row - distance + rows, rows) * inner + (column ^ c)
        return move(which, target, distance * inner + c, down_send, down_recv)

    def up(which, distance, c):
        target = lax.rem(row + distance, rows) * inner + (column ^ c)
        return move(which, target, distance * inner + c, up_send, up_recv)

    def near(which, c):
        return move(which, row * inner + (column ^ c), c, near_send, near_recv)

    def start_down(distance, kinds):
        for which in kinds:
            for c in turns:
                down(which, distance, c).start()

    def start_up(distance, kinds):
        for which in kinds:
            for c in turns:
                up(which, distance, c).start()

    def await_up(distance, c):
        pl.semaphore_wait(present.at[(row + distance) * inner + (column ^ c)], 1)

    @pl.when(row > 0)
    def _():
        start_down(row, (0, 1))

    for u in range(1, rows - 1):

        @pl.when(u < row - 1)
        def _():
            start_down(u, (0, 1))

        @pl.when(u == row - 1)
        def _():
            start_down(u, (0,))

    early = [2 * (column // 2) ^ c for c in range(inner)] if inner == 4 else list(range(inner))
    for u in range(1, rows):

        @pl.when(row + u < rows)
        def _():
            for c in early:
                if u > 1:
                    await_up(u, c)
                else:

                    @pl.when(row != gate_low)
                    def _():
                        await_up(u, c)

                if u > 1:
                    up(0, u, c).start()
                else:

                    @pl.when(row > 0)
                    def _():
                        up(0, u, c).start()

        if u > 1:

            @pl.when((row == 0) & (row + u < rows))
            def _():
                start_up(u, (1,))

    for load in loads:
        load.start()
    for c in range(1, inner):

        @pl.when((column ^ c) > column)
        def _():
            pl.semaphore_wait(present.at[row * inner + (column ^ c)], 1)

        for which in (0, 1):
            near(which, c).start()

    def start_rest():
        @pl.when(row > 1)
        def _():
            start_down(row - 1, (1,))

        for u in range(rows - 1, 0, -1):

            @pl.when((row > 0) & (row + u < rows))
            def _():
                start_up(u, (1,))

        if rows > 1:

            @pl.when(row == 0)
            def _():
                start_up(1, (0, 1))

    for load in loads:
        load.wait()

    lanes = lax.broadcasted_iota(jnp.int32, (1, BLOCK), 1)
    scores_own[...] = jnp.zeros_like(scores_own)

    def decode(p, carry):
        seq_id = (first_pair + p) // KVH
        length = lengths_ref[seq_id]
        rows = queries[p].reshape(steps * group, width)
        scores = (
            lax.dot_general(
                rows, keys[p], (((1,), (1,)), ((), ())), preferred_element_type=jnp.float32
            )
            * scaling
        )
        limits = []
        for b in range(blocks):
            limit = jnp.where(keep_ref[seq_id, b] > 0, length - b * BLOCK, 0)
            limits.append(lanes < limit)
        visible = jnp.concatenate([jnp.where(v, 0.0, -jnp.inf) for v in limits], axis=1)
        scores = scores + visible
        rows32 = rows.astype(jnp.float32)
        row_step = lax.broadcasted_iota(jnp.int32, (steps * group, 1), 0) // group
        own = []
        highest = jnp.max(scores, axis=1, keepdims=True)
        for j in range(steps):
            key_row = new_keys[p, j : j + 1].astype(jnp.float32)
            own_j = jnp.sum(rows32 * key_row, axis=1, keepdims=True) * scaling
            own_j = jnp.where(j <= row_step, own_j, -jnp.inf)
            own.append(own_j)
            highest = jnp.maximum(highest, own_j)
        weights = jnp.exp(scores - highest)
        total = jnp.sum(weights, axis=1, keepdims=True)
        summed = jnp.dot(
            weights.astype(jnp.bfloat16), values[p], preferred_element_type=jnp.float32
        )
        for j in range(steps):
            own_weight = jnp.exp(own[j] - highest)
            total = total + own_weight
            value_row = new_values[p, j : j + 1].astype(jnp.float32)
            summed = summed + own_weight.astype(jnp.bfloat16).astype(jnp.float32) * value_row
        attended_own[p] = (summed / total).astype(jnp.bfloat16).reshape(steps, group, width)
        mass = jnp.sum(weights / total, axis=0, keepdims=True) / group
        line = jnp.zeros((1, BLOCK), jnp.float32)
        for b in range(blocks):
            piece = jnp.sum(mass[:, b * BLOCK : (b + 1) * BLOCK], axis=1, keepdims=True)
            line = line + jnp.where(lanes == b, piece, 0.0)
        scores_own[pl.ds(p, 1), :] = line
        return carry

    lax.fori_loop(0, pairs, decode, 0)

    factor = scaling * math.log2(math.e)
    per_chunk = chunk // BLOCK
    gap = lax.broadcasted_iota(jnp.int32, (BLOCK, win), 1) - lax.broadcasted_iota(
        jnp.int32, (BLOCK, win), 0
    )
    row_block = lax.broadcasted_iota(jnp.int32, (blocks * 8, BLOCK), 0) // 8
    in_block = row_block == lax.broadcasted_iota(jnp.int32, (blocks * 8, BLOCK), 1)

    def one_pair(p, carry):
        seq_id = (first_pair + p) // KVH
        start = lengths_ref[seq_id] - win
        mass_acc[...] = jnp.zeros_like(mass_acc)

        def one_head(g, carry):
            wide = window[p, g].astype(jnp.float32) * factor
            high = wide.astype(jnp.bfloat16)
            low = (wide - high.astype(jnp.float32)).astype(jnp.bfloat16)
            scaled_queries[...] = jnp.concatenate([high.T, low.T], axis=0)

            def one_chunk(c, carry):
                base = pl.multiple_of(c * chunk, chunk)
                tile = keys[p, pl.ds(base, chunk), :]
                doubled = jnp.concatenate([tile, tile], axis=1)
                scores = jnp.dot(doubled, scaled_queries[...], preferred_element_type=jnp.float32)
                for i in range(per_chunk):
                    b = c * per_chunk + i
                    part_scores = jnp.where(
                        gap >= b * BLOCK - start, scores[i * BLOCK : (i + 1) * BLOCK], LOW
                    )
                    stacked = part_scores.reshape(BLOCK // 8, 8, win)
                    top = jnp.max(stacked, axis=0)
                    total = jnp.sum(jnp.exp2(stacked - top[None]), axis=0)
                    kept = keep_ref[seq_id, b] > 0
                    spot = pl.ds(pl.multiple_of(b * 8, 8), 8)
                    block_max[spot, :] = jnp.where(kept, top, LOW)
                    block_sum[spot, :] = jnp.where(kept, total, 0.0)
                return carry

            lax.fori_loop(0, tokens // chunk, one_chunk, 0)
            highest = jnp.max(block_max[...], axis=0, keepdims=True)
            shares = block_sum[...] * jnp.exp2(block_max[...] - highest)
            mass_acc[...] += shares / jnp.sum(shares, axis=0, keepdims=True)
            return carry

        lax.fori_loop(0, group, one_head, 0)
        row_mass = jnp.sum(mass_acc[...], axis=1, keepdims=True)
        prior = jnp.sum(jnp.where(in_block, row_mass, 0.0), axis=0, keepdims=True) / group
        line = prior.astype(jnp.bfloat16).astype(jnp.float32)
        scores_own[pl.ds(p, 1), :] = scores_own[pl.ds(p, 1), :] + line
        return carry

    lax.fori_loop(0, pairs, one_pair, 0)

    results = ((attended_own, attended_out), (scores_own, scores_all))
    low = row < half

    def along(i, u):
        own, landing = results[i]
        return pltpu.make_async_remote_copy(
            src_ref=own,
            dst_ref=landing.at[row, column],
            send_sem=along_send.at[i, u],
            recv_sem=along_recv.at[i, u],
            device_id=(group_me, lax.rem(row + u, rows) * inner + column),
            device_id_type=MESH,
        )

    def relay(i, upward, target):
        landing = results[i][1]
        block = landing.at[pl.ds(0, half) if upward else pl.ds(half, rows - half), column]
        return pltpu.make_async_remote_copy(
            src_ref=block,
            dst_ref=block,
            send_sem=relay_send.at[i, target],
            recv_sem=relay_recv.at[i],
            device_id=(group_me, target * inner + column),
            device_id_type=MESH,
        )

    across = [
        pltpu.make_async_remote_copy(
            src_ref=landing.at[:, column],
            dst_ref=landing.at[:, column],
            send_sem=across_send.at[i, c],
            recv_sem=across_recv.at[i, c],
            device_id=(group_me, row * inner + (column ^ c)),
            device_id_type=MESH,
        )
        for c in range(1, inner)
        for i, (own, landing) in enumerate(results)
    ]
    kept_here = [
        pltpu.make_async_copy(own, landing.at[row, column], local_sems.at[i])
        for i, (own, landing) in enumerate(results)
    ]
    for u in range(1, rows):
        target = lax.rem(row + u, rows)

        @pl.when((low == (target < half)) | (target == jnp.where(low, half, half - 1)))
        def _():
            for i in range(2):
                along(i, u).start()

    start_rest()
    for copy in kept_here:
        copy.start()
    for copy in kept_here:
        copy.wait()
    for u in range(1, rows):
        source = lax.rem(row + rows - u, rows)

        @pl.when((low == (source < half)) | (row == jnp.where(source < half, half, half - 1)))
        def _():
            for i in range(2):
                along(i, u).wait_recv()

    upper, lower = range(half + 1, rows), range(0, half - 1)
    for upward, gate, targets in ((True, half, upper), (False, half - 1, lower)):
        for target in targets:

            @pl.when(row == gate)
            def _():
                for i in range(2):
                    relay(i, upward, target).start()

            @pl.when(row == target)
            def _():
                for i in range(2):
                    relay(i, upward, target).wait_recv()

    for copy in across:
        copy.start()
    for copy in across:
        copy.wait()
    for upward, gate, targets in ((True, half, upper), (False, half - 1, lower)):
        for target in targets:

            @pl.when(row == gate)
            def _():
                for i in range(2):
                    relay(i, upward, target).wait_send()

    for u in range(1, rows):
        target = lax.rem(row + u, rows)

        @pl.when((low == (target < half)) | (target == jnp.where(low, half, half - 1)))
        def _():
            for i in range(2):
                along(i, u).wait_send()

    for c in range(1, inner):
        for which in (0, 1):
            near(which, c).wait()
    for u in range(1, rows):
        for make, sends, receives in (
            (down, row >= u, row + u < rows),
            (up, row + u < rows, row >= u),
        ):

            @pl.when(sends)
            def _():
                for which in (0, 1):
                    for c in range(inner):
                        make(which, u, c).wait_send()

            @pl.when(receives)
            def _():
                for which in (0, 1):
                    for c in range(inner):
                        make(which, u, c).wait_recv()


def settle(n, pieces, keys, values, attended, scores, *rest):
    cache_keys, cache_values, attended_out, scores_out, turned_scores, sems = rest
    me = lax.axis_index("seq")
    here = scores_out.shape[0]
    step = keys.shape[0] // pieces
    stores = []
    for source, target in ((keys, cache_keys), (values, cache_values)):
        for i in range(pieces):
            spot = pl.ds(i * step, step)
            stores.append(
                pltpu.make_async_copy(source.at[spot], target.at[spot], sems.at[len(stores)])
            )
    stores.append(pltpu.make_async_copy(attended, attended_out, sems.at[len(stores)]))
    for store in stores:
        store.start()
    flat = scores[...].reshape(math.prod(scores.shape[:-1]), BLOCK)
    turned = pltpu.roll(flat, lax.rem(BLOCK - me * here, BLOCK), 1)
    turned_scores[...] = turned.T[:here]
    stores.append(pltpu.make_async_copy(turned_scores, scores_out, sems.at[len(stores)]))
    stores[-1].start()
    for store in stores:
        store.wait()


def local(n, *args):
    keys, values, window, queries, new_keys, new_values, lengths, keep = args
    pairs, tokens, width = keys.shape
    part = tokens // n
    blocks = tokens // BLOCK
    win = window.shape[2]
    every = n * pairs
    inner = 4 if n % 4 == 0 else 1
    vmem = pl.BlockSpec(memory_space=pltpu.VMEM)
    hbm = pl.BlockSpec(memory_space=pltpu.HBM)
    free = pl.BlockSpec(memory_space=pl.ANY)
    bf16, f32 = jnp.bfloat16, jnp.float32
    moved = pl.pallas_call(
        functools.partial(kernel, n, min(512, tokens), inner),
        out_shape=(
            pltpu.VMEM((every, part, width), bf16),
            pltpu.VMEM((every, part, width), bf16),
            pltpu.VMEM((n // inner, inner, pairs) + queries.shape[1:], bf16),
            pltpu.VMEM((n // inner, inner, pairs, BLOCK), f32),
        ),
        in_specs=[hbm] * 8,
        out_specs=(vmem,) * 4,
        scratch_shapes=[
            pltpu.VMEM(keys.shape, bf16),
            pltpu.VMEM(values.shape, bf16),
            pltpu.VMEM(window.shape, bf16),
            pltpu.VMEM((pairs,) + queries.shape[1:], bf16),
            pltpu.VMEM((pairs,) + new_keys.shape[1:], bf16),
            pltpu.VMEM((pairs,) + new_values.shape[1:], bf16),
            pltpu.SMEM(lengths.shape, jnp.int32),
            pltpu.SMEM(keep.shape, jnp.int32),
            pltpu.VMEM((2 * width, win), bf16),
            pltpu.VMEM((blocks * 8, win), f32),
            pltpu.VMEM((blocks * 8, win), f32),
            pltpu.VMEM((blocks * 8, win), f32),
            pltpu.VMEM((pairs,) + queries.shape[1:], bf16),
            pltpu.VMEM((pairs, BLOCK), f32),
            pltpu.SemaphoreType.DMA((10,)),
        ]
        + [pltpu.SemaphoreType.REGULAR((n,))]
        + [pltpu.SemaphoreType.DMA((2, n))] * 4
        + [pltpu.SemaphoreType.DMA((2, inner))] * 2
        + [pltpu.SemaphoreType.DMA((2, n))] * 3
        + [pltpu.SemaphoreType.DMA((2,))]
        + [pltpu.SemaphoreType.DMA((2, n))] * 2,
        compiler_params=pltpu.CompilerParams(
            collective_id=0, has_side_effects=True, vmem_limit_bytes=LIMIT
        ),
    )(*(pltpu.with_memory_space_constraint(a, pltpu.HBM) for a in args))
    pieces = math.gcd(every, 8)
    cache_keys, cache_values, attended, scores = pl.pallas_call(
        functools.partial(settle, n, pieces),
        out_shape=(
            jax.ShapeDtypeStruct((every, part, width), bf16),
            jax.ShapeDtypeStruct((every, part, width), bf16),
            jax.ShapeDtypeStruct(moved[2].shape, bf16),
            jax.ShapeDtypeStruct((part // BLOCK, every), f32),
        ),
        in_specs=[vmem] * 4,
        out_specs=(free,) * 4,
        scratch_shapes=[
            pltpu.VMEM((part // BLOCK, every), f32),
            pltpu.SemaphoreType.DMA((2 * pieces + 2,)),
        ],
        compiler_params=pltpu.CompilerParams(vmem_limit_bytes=LIMIT),
    )(*moved)
    return cache_keys, cache_values, attended.reshape((every,) + queries.shape[1:]), scores.T


def solution(mesh):
    placed = (
        P(("groups", "seq"), None, None),
        P(("groups", "seq"), None, None),
        P(("groups", "seq"), None, None, None),
        P("groups", None, None, None),
        P("groups", None, None),
        P("groups", None, None),
        P("groups"),
        P("groups", None),
    )
    return jax.shard_map(
        functools.partial(local, mesh.shape["seq"]),
        mesh=mesh,
        in_specs=placed,
        out_specs=(
            P("groups", "seq", None),
            P("groups", "seq", None),
            P("groups", None, None, None),
            P("groups", "seq"),
        ),
        check_vma=False,
    )
```

```python
import functools
import math

import jax
import jax.numpy as jnp
from jax import lax
from jax.experimental import pallas as pl
from jax.experimental.pallas import tpu as pltpu
from jax.sharding import PartitionSpec as P

KVH = 8
BLOCK = 128
LOW = -1e30
LIMIT = 32 * 1024 * 1024
MESH = pl.DeviceIdType.MESH


def kernel(
    n,
    chunk,
    inner,
    keys_hbm,
    values_hbm,
    window_hbm,
    queries_hbm,
    new_keys_hbm,
    new_values_hbm,
    lengths_hbm,
    keep_hbm,
    cache_keys,
    cache_values,
    attended_out,
    scores_all,
    keys,
    values,
    window,
    queries,
    new_keys,
    new_values,
    lengths_ref,
    keep_ref,
    scaled_queries,
    block_max,
    block_sum,
    mass_acc,
    attended_own,
    scores_own,
    local_sems,
    present,
    up_send,
    up_recv,
    down_send,
    down_recv,
    near_send,
    near_recv,
    along_send,
    along_recv,
    relay_send,
    relay_recv,
    across_send,
    across_recv,
):
    group_me = lax.axis_index("groups")
    me = lax.axis_index("seq")
    pairs, tokens, width = keys_hbm.shape
    part = tokens // n
    group = window_hbm.shape[1]
    win = window_hbm.shape[2]
    steps = queries_hbm.shape[1]
    blocks = tokens // BLOCK
    first_pair = me * pairs
    scaling = 1.0 / math.sqrt(width)
    rows = n // inner
    row, column = me // inner, lax.rem(me, inner)

    half = rows // 2
    gate_low, gate_high = half - 1, half
    barrier = pltpu.get_barrier_semaphore()
    for k in range(1, n):

        @pl.when(me + k < n)
        def _():
            pl.semaphore_signal(
                barrier, inc=1, device_id=(group_me, me + k), device_id_type=MESH
            )

    loads = [
        pltpu.make_async_copy(keys_hbm, keys, local_sems.at[0]),
        pltpu.make_async_copy(values_hbm, values, local_sems.at[1]),
        pltpu.make_async_copy(window_hbm, window, local_sems.at[2]),
        pltpu.make_async_copy(queries_hbm.at[pl.ds(first_pair, pairs)], queries, local_sems.at[3]),
        pltpu.make_async_copy(new_keys_hbm.at[pl.ds(first_pair, pairs)], new_keys, local_sems.at[4]),
        pltpu.make_async_copy(
            new_values_hbm.at[pl.ds(first_pair, pairs)], new_values, local_sems.at[5]
        ),
        pltpu.make_async_copy(
            keys_hbm.at[:, pl.ds(me * part, part), :],
            cache_keys.at[pl.ds(first_pair, pairs)],
            local_sems.at[6],
        ),
        pltpu.make_async_copy(
            values_hbm.at[:, pl.ds(me * part, part), :],
            cache_values.at[pl.ds(first_pair, pairs)],
            local_sems.at[7],
        ),
        pltpu.make_async_copy(lengths_hbm, lengths_ref, local_sems.at[8]),
        pltpu.make_async_copy(keep_hbm, keep_ref, local_sems.at[9]),
    ]
    if rows > 1:

        @pl.when(row == gate_high)
        def _():
            for c in range(inner):
                pl.semaphore_signal(
                    barrier, inc=1, device_id=(group_me, gate_low * inner + c), device_id_type=MESH
                )

        @pl.when(row == gate_low)
        def _():
            pl.semaphore_wait(barrier, me + inner)

    @pl.when((me > 0) & (row != gate_low))
    def _():
        pl.semaphore_wait(barrier, me)

    for k in range(1, n):

        @pl.when((me >= k) & ((row != gate_high) | ((me - k) // inner != gate_low)))
        def _():
            pl.semaphore_signal(
                present.at[me], inc=1, device_id=(group_me, me - k), device_id_type=MESH
            )

    if inner == 4:
        flip = 2 * lax.rem(column, 2)
        turns = [flip, 2 - flip, 1 + flip, 3 - flip]
    else:
        turns = list(range(inner))

    def move(which, target, spot, send, recv):
        src, dst = ((keys_hbm, cache_keys), (values_hbm, cache_values))[which]
        return pltpu.make_async_remote_copy(
            src_ref=src.at[:, pl.ds(target * part, part), :],
            dst_ref=dst.at[pl.ds(first_pair, pairs)],
            send_sem=send.at[which, spot],
            recv_sem=recv.at[which, spot],
            device_id=(group_me, target),
            device_id_type=MESH,
        )

    def down(which, distance, c):
        target = lax.rem(row - distance + rows, rows) * inner + (column ^ c)
        return move(which, target, distance * inner + c, down_send, down_recv)

    def up(which, distance, c):
        target = lax.rem(row + distance, rows) * inner + (column ^ c)
        return move(which, target, distance * inner + c, up_send, up_recv)

    def near(which, c):
        return move(which, row * inner + (column ^ c), c, near_send, near_recv)

    def start_down(distance, kinds):
        for which in kinds:
            for c in turns:
                down(which, distance, c).start()

    def start_up(distance, kinds):
        for which in kinds:
            for c in turns:
                up(which, distance, c).start()

    def await_up(distance, c):
        pl.semaphore_wait(present.at[(row + distance) * inner + (column ^ c)], 1)

    @pl.when((row > 1) & (row == gate_high))
    def _():
        start_down(row - 1, (0,))

    @pl.when(row > 0)
    def _():
        start_down(row, (0, 1))

    for u in range(1, rows - 1):

        @pl.when(u < row - 1)
        def _():
            start_down(u, (0, 1))

        @pl.when((u == row - 1) & (row != gate_high))
        def _():
            start_down(u, (0,))

    early = [2 * (column // 2) ^ c for c in range(inner)] if inner == 4 else list(range(inner))
    for u in range(1, rows):

        @pl.when(row + u < rows)
        def _():
            for c in early:
                if u > 1:
                    await_up(u, c)
                else:

                    @pl.when(row != gate_low)
                    def _():
                        await_up(u, c)

                if u > 1:
                    up(0, u, c).start()
                else:

                    @pl.when(row > 0)
                    def _():
                        up(0, u, c).start()

        if u > 1:

            @pl.when((row == 0) & (row + u < rows))
            def _():
                start_up(u, (1,))

    for load in loads:
        load.start()
    for c in range(1, inner):

        @pl.when((column ^ c) > column)
        def _():
            pl.semaphore_wait(present.at[row * inner + (column ^ c)], 1)

        for which in (0, 1):
            near(which, c).start()

    def start_rest():
        @pl.when(row > 1)
        def _():
            start_down(row - 1, (1,))

        for u in range(rows - 1, 0, -1):

            @pl.when((row > 0) & (row + u < rows))
            def _():
                start_up(u, (1,))

        if rows > 1:

            @pl.when(row == 0)
            def _():
                start_up(1, (0, 1))

    for load in loads:
        load.wait()

    lanes = lax.broadcasted_iota(jnp.int32, (1, BLOCK), 1)
    scores_own[...] = jnp.zeros_like(scores_own)

    def decode(p, carry):
        seq_id = (first_pair + p) // KVH
        length = lengths_ref[seq_id]
        rows = queries[p].reshape(steps * group, width)
        scores = (
            lax.dot_general(
                rows, keys[p], (((1,), (1,)), ((), ())), preferred_element_type=jnp.float32
            )
            * scaling
        )
        limits = []
        for b in range(blocks):
            limit = jnp.where(keep_ref[seq_id, b] > 0, length - b * BLOCK, 0)
            limits.append(lanes < limit)
        visible = jnp.concatenate([jnp.where(v, 0.0, -jnp.inf) for v in limits], axis=1)
        scores = scores + visible
        rows32 = rows.astype(jnp.float32)
        row_step = lax.broadcasted_iota(jnp.int32, (steps * group, 1), 0) // group
        own = []
        highest = jnp.max(scores, axis=1, keepdims=True)
        for j in range(steps):
            key_row = new_keys[p, j : j + 1].astype(jnp.float32)
            own_j = jnp.sum(rows32 * key_row, axis=1, keepdims=True) * scaling
            own_j = jnp.where(j <= row_step, own_j, -jnp.inf)
            own.append(own_j)
            highest = jnp.maximum(highest, own_j)
        weights = jnp.exp(scores - highest)
        total = jnp.sum(weights, axis=1, keepdims=True)
        summed = jnp.dot(
            weights.astype(jnp.bfloat16), values[p], preferred_element_type=jnp.float32
        )
        for j in range(steps):
            own_weight = jnp.exp(own[j] - highest)
            total = total + own_weight
            value_row = new_values[p, j : j + 1].astype(jnp.float32)
            summed = summed + own_weight.astype(jnp.bfloat16).astype(jnp.float32) * value_row
        attended_own[p] = (summed / total).astype(jnp.bfloat16).reshape(steps, group, width)
        mass = jnp.sum(weights / total, axis=0, keepdims=True) / group
        line = jnp.zeros((1, BLOCK), jnp.float32)
        for b in range(blocks):
            piece = jnp.sum(mass[:, b * BLOCK : (b + 1) * BLOCK], axis=1, keepdims=True)
            line = line + jnp.where(lanes == b, piece, 0.0)
        scores_own[pl.ds(p, 1), :] = line
        return carry

    lax.fori_loop(0, pairs, decode, 0)

    factor = scaling * math.log2(math.e)
    per_chunk = chunk // BLOCK
    gap = lax.broadcasted_iota(jnp.int32, (BLOCK, win), 1) - lax.broadcasted_iota(
        jnp.int32, (BLOCK, win), 0
    )
    row_block = lax.broadcasted_iota(jnp.int32, (blocks * 8, BLOCK), 0) // 8
    in_block = row_block == lax.broadcasted_iota(jnp.int32, (blocks * 8, BLOCK), 1)

    def one_pair(p, carry):
        seq_id = (first_pair + p) // KVH
        start = lengths_ref[seq_id] - win
        mass_acc[...] = jnp.zeros_like(mass_acc)

        def one_head(g, carry):
            wide = window[p, g].astype(jnp.float32) * factor
            high = wide.astype(jnp.bfloat16)
            low = (wide - high.astype(jnp.float32)).astype(jnp.bfloat16)
            scaled_queries[...] = jnp.concatenate([high.T, low.T], axis=0)

            def one_chunk(c, carry):
                base = pl.multiple_of(c * chunk, chunk)
                tile = keys[p, pl.ds(base, chunk), :]
                doubled = jnp.concatenate([tile, tile], axis=1)
                scores = jnp.dot(doubled, scaled_queries[...], preferred_element_type=jnp.float32)
                for i in range(per_chunk):
                    b = c * per_chunk + i
                    part_scores = jnp.where(
                        gap >= b * BLOCK - start, scores[i * BLOCK : (i + 1) * BLOCK], LOW
                    )
                    stacked = part_scores.reshape(BLOCK // 8, 8, win)
                    top = jnp.max(stacked, axis=0)
                    total = jnp.sum(jnp.exp2(stacked - top[None]), axis=0)
                    kept = keep_ref[seq_id, b] > 0
                    spot = pl.ds(pl.multiple_of(b * 8, 8), 8)
                    block_max[spot, :] = jnp.where(kept, top, LOW)
                    block_sum[spot, :] = jnp.where(kept, total, 0.0)
                return carry

            lax.fori_loop(0, tokens // chunk, one_chunk, 0)
            highest = jnp.max(block_max[...], axis=0, keepdims=True)
            shares = block_sum[...] * jnp.exp2(block_max[...] - highest)
            mass_acc[...] += shares / jnp.sum(shares, axis=0, keepdims=True)
            return carry

        lax.fori_loop(0, group, one_head, 0)
        row_mass = jnp.sum(mass_acc[...], axis=1, keepdims=True)
        prior = jnp.sum(jnp.where(in_block, row_mass, 0.0), axis=0, keepdims=True) / group
        line = prior.astype(jnp.bfloat16).astype(jnp.float32)
        scores_own[pl.ds(p, 1), :] = scores_own[pl.ds(p, 1), :] + line
        return carry

    lax.fori_loop(0, pairs, one_pair, 0)

    results = ((attended_own, attended_out), (scores_own, scores_all))
    low = row < half

    def along(i, u):
        own, landing = results[i]
        return pltpu.make_async_remote_copy(
            src_ref=own,
            dst_ref=landing.at[row, column],
            send_sem=along_send.at[i, u],
            recv_sem=along_recv.at[i, u],
            device_id=(group_me, lax.rem(row + u, rows) * inner + column),
            device_id_type=MESH,
        )

    def relay(i, upward, target):
        landing = results[i][1]
        block = landing.at[pl.ds(0, half) if upward else pl.ds(half, rows - half), column]
        return pltpu.make_async_remote_copy(
            src_ref=block,
            dst_ref=block,
            send_sem=relay_send.at[i, target],
            recv_sem=relay_recv.at[i],
            device_id=(group_me, target * inner + column),
            device_id_type=MESH,
        )

    across = [
        pltpu.make_async_remote_copy(
            src_ref=landing.at[:, column],
            dst_ref=landing.at[:, column],
            send_sem=across_send.at[i, c],
            recv_sem=across_recv.at[i, c],
            device_id=(group_me, row * inner + (column ^ c)),
            device_id_type=MESH,
        )
        for c in range(1, inner)
        for i, (own, landing) in enumerate(results)
    ]
    kept_here = [
        pltpu.make_async_copy(own, landing.at[row, column], local_sems.at[i])
        for i, (own, landing) in enumerate(results)
    ]
    for u in range(1, rows):
        target = lax.rem(row + u, rows)

        @pl.when((low == (target < half)) | (target == jnp.where(low, half, half - 1)))
        def _():
            for i in range(2):
                along(i, u).start()

    start_rest()
    for copy in kept_here:
        copy.start()
    for copy in kept_here:
        copy.wait()
    for u in range(1, rows):
        source = lax.rem(row + rows - u, rows)

        @pl.when((low == (source < half)) | (row == jnp.where(source < half, half, half - 1)))
        def _():
            for i in range(2):
                along(i, u).wait_recv()

    upper, lower = range(half + 1, rows), range(0, half - 1)
    for upward, gate, targets in ((True, half, upper), (False, half - 1, lower)):
        for target in targets:

            @pl.when(row == gate)
            def _():
                for i in range(2):
                    relay(i, upward, target).start()

            @pl.when(row == target)
            def _():
                for i in range(2):
                    relay(i, upward, target).wait_recv()

    for copy in across:
        copy.start()
    for copy in across:
        copy.wait()
    for upward, gate, targets in ((True, half, upper), (False, half - 1, lower)):
        for target in targets:

            @pl.when(row == gate)
            def _():
                for i in range(2):
                    relay(i, upward, target).wait_send()

    for u in range(1, rows):
        target = lax.rem(row + u, rows)

        @pl.when((low == (target < half)) | (target == jnp.where(low, half, half - 1)))
        def _():
            for i in range(2):
                along(i, u).wait_send()

    for c in range(1, inner):
        for which in (0, 1):
            near(which, c).wait()
    for u in range(1, rows):
        for make, sends, receives in (
            (down, row >= u, row + u < rows),
            (up, row + u < rows, row >= u),
        ):

            @pl.when(sends)
            def _():
                for which in (0, 1):
                    for c in range(inner):
                        make(which, u, c).wait_send()

            @pl.when(receives)
            def _():
                for which in (0, 1):
                    for c in range(inner):
                        make(which, u, c).wait_recv()


def settle(n, pieces, keys, values, attended, scores, *rest):
    cache_keys, cache_values, attended_out, scores_out, turned_scores, sems = rest
    me = lax.axis_index("seq")
    here = scores_out.shape[0]
    step = keys.shape[0] // pieces
    stores = []
    for source, target in ((keys, cache_keys), (values, cache_values)):
        for i in range(pieces):
            spot = pl.ds(i * step, step)
            stores.append(
                pltpu.make_async_copy(source.at[spot], target.at[spot], sems.at[len(stores)])
            )
    stores.append(pltpu.make_async_copy(attended, attended_out, sems.at[len(stores)]))
    for store in stores:
        store.start()
    flat = scores[...].reshape(math.prod(scores.shape[:-1]), BLOCK)
    turned = pltpu.roll(flat, lax.rem(BLOCK - me * here, BLOCK), 1)
    turned_scores[...] = turned.T[:here]
    stores.append(pltpu.make_async_copy(turned_scores, scores_out, sems.at[len(stores)]))
    stores[-1].start()
    for store in stores:
        store.wait()


def local(n, *args):
    keys, values, window, queries, new_keys, new_values, lengths, keep = args
    pairs, tokens, width = keys.shape
    part = tokens // n
    blocks = tokens // BLOCK
    win = window.shape[2]
    every = n * pairs
    inner = 4 if n % 4 == 0 else 1
    vmem = pl.BlockSpec(memory_space=pltpu.VMEM)
    hbm = pl.BlockSpec(memory_space=pltpu.HBM)
    free = pl.BlockSpec(memory_space=pl.ANY)
    bf16, f32 = jnp.bfloat16, jnp.float32
    moved = pl.pallas_call(
        functools.partial(kernel, n, min(512, tokens), inner),
        out_shape=(
            pltpu.VMEM((every, part, width), bf16),
            pltpu.VMEM((every, part, width), bf16),
            pltpu.VMEM((n // inner, inner, pairs) + queries.shape[1:], bf16),
            pltpu.VMEM((n // inner, inner, pairs, BLOCK), f32),
        ),
        in_specs=[hbm] * 8,
        out_specs=(vmem,) * 4,
        scratch_shapes=[
            pltpu.VMEM(keys.shape, bf16),
            pltpu.VMEM(values.shape, bf16),
            pltpu.VMEM(window.shape, bf16),
            pltpu.VMEM((pairs,) + queries.shape[1:], bf16),
            pltpu.VMEM((pairs,) + new_keys.shape[1:], bf16),
            pltpu.VMEM((pairs,) + new_values.shape[1:], bf16),
            pltpu.SMEM(lengths.shape, jnp.int32),
            pltpu.SMEM(keep.shape, jnp.int32),
            pltpu.VMEM((2 * width, win), bf16),
            pltpu.VMEM((blocks * 8, win), f32),
            pltpu.VMEM((blocks * 8, win), f32),
            pltpu.VMEM((blocks * 8, win), f32),
            pltpu.VMEM((pairs,) + queries.shape[1:], bf16),
            pltpu.VMEM((pairs, BLOCK), f32),
            pltpu.SemaphoreType.DMA((10,)),
        ]
        + [pltpu.SemaphoreType.REGULAR((n,))]
        + [pltpu.SemaphoreType.DMA((2, n))] * 4
        + [pltpu.SemaphoreType.DMA((2, inner))] * 2
        + [pltpu.SemaphoreType.DMA((2, n))] * 3
        + [pltpu.SemaphoreType.DMA((2,))]
        + [pltpu.SemaphoreType.DMA((2, n))] * 2,
        compiler_params=pltpu.CompilerParams(
            collective_id=0, has_side_effects=True, vmem_limit_bytes=LIMIT
        ),
    )(*(pltpu.with_memory_space_constraint(a, pltpu.HBM) for a in args))
    pieces = math.gcd(every, 2)
    cache_keys, cache_values, attended, scores = pl.pallas_call(
        functools.partial(settle, n, pieces),
        out_shape=(
            jax.ShapeDtypeStruct((every, part, width), bf16),
            jax.ShapeDtypeStruct((every, part, width), bf16),
            jax.ShapeDtypeStruct(moved[2].shape, bf16),
            jax.ShapeDtypeStruct((part // BLOCK, every), f32),
        ),
        in_specs=[vmem] * 4,
        out_specs=(free,) * 4,
        scratch_shapes=[
            pltpu.VMEM((part // BLOCK, every), f32),
            pltpu.SemaphoreType.DMA((2 * pieces + 2,)),
        ],
        compiler_params=pltpu.CompilerParams(vmem_limit_bytes=LIMIT),
    )(*moved)
    return cache_keys, cache_values, attended.reshape((every,) + queries.shape[1:]), scores.T


def solution(mesh):
    placed = (
        P(("groups", "seq"), None, None),
        P(("groups", "seq"), None, None),
        P(("groups", "seq"), None, None, None),
        P("groups", None, None, None),
        P("groups", None, None),
        P("groups", None, None),
        P("groups"),
        P("groups", None),
    )
    return jax.shard_map(
        functools.partial(local, mesh.shape["seq"]),
        mesh=mesh,
        in_specs=placed,
        out_specs=(
            P("groups", "seq", None),
            P("groups", "seq", None),
            P("groups", None, None, None),
            P("groups", "seq"),
        ),
        check_vma=False,
    )
```
